128 devices in a mesh: rad: 16 (over y, x), ang: 8 (over z, core).
Axes of the slice: x: 4, y: 4, z: 4, core: 2. Of those that a mesh axis runs over, the one named last changes fastest.
Arguments:
- density: float32 [3, 1024, 256, 512], P(None, 'rad', 'ang'), may hold values from -13 to 13
Outputs:
- potential: float32 [3, 1024, 256, 512], P(None, 'rad', 'ang')
The draws below stay inside these ranges and needn't reach their ends.
All inputs are finite; a program needn't handle non-finite values.
Results may differ from the reference program's by a relative error of at most 0.0003.
Values sent between devices are 32-bit elements; how exact they have to be, the bound alone decides.
A program may use at most 128 MiB of HBM per device.

```python
import math
import jax
import jax.numpy as jnp
from jax import lax

LMAX = 12
NPHI = 512
FIELDS = 3
NR = 1024
NTH = 256


def draw_density(key, part):
    key_scale, key_noise = jax.random.split(jax.random.fold_in(key, 11))
    scales = jnp.exp(jax.random.uniform(key_scale, (FIELDS, NR, 1, 1), jnp.float32, math.log(0.5), math.log(2.0)))
    noise = jax.random.truncated_normal(key_noise, -3.0, 3.0, (FIELDS, NR, NTH, NPHI), jnp.float32)
    rough = (noise - jnp.roll(noise, 1, axis=1)) * math.sqrt(0.5)
    return scales * rough


def setup_inputs(seed: int = 0) -> dict:
    arg_keys = jax.random.split(jax.random.key(seed), 2)
    return {
        "density": draw_density(jax.random.fold_in(arg_keys[1], 71), 0),
    }


INNER = 0.5
COUPLING = 2000.0

def legendre_table(polar_angle):
    cos_theta = jnp.cos(polar_angle)
    sine_theta = jnp.sin(polar_angle)
    values_lm = {}
    values_lm[0, 0] = jnp.full_like(polar_angle, 1.0 / math.sqrt(4.0 * math.pi))
    for m in range(1, LMAX + 1):
        values_lm[m, m] = math.sqrt((2.0 * m + 1.0) / (2.0 * m)) * sine_theta * values_lm[m - 1, m - 1]
    for m in range(0, LMAX):
        values_lm[m + 1, m] = math.sqrt(2.0 * m + 3.0) * cos_theta * values_lm[m, m]
    for m in range(0, LMAX + 1):
        for l in range(m + 2, LMAX + 1):
            coef_a = math.sqrt((4.0 * l * l - 1.0) / (l * l - m * m))
            coef_b = math.sqrt(((l - 1.0) ** 2 - m * m) / (4.0 * (l - 1.0) ** 2 - 1.0))
            values_lm[l, m] = coef_a * (cos_theta * values_lm[l - 1, m] - coef_b * values_lm[l - 2, m])
    degree_rows = []
    for l in range(LMAX + 1):
        columns = []
        for k in range(2 * LMAX + 1):
            m = (k + 1) // 2
            columns.append(values_lm[l, m] if m <= l else jnp.zeros_like(polar_angle))
        degree_rows.append(jnp.stack(columns, -1))
    return jnp.stack(degree_rows, 1)

def fourier_table(phi_cells):
    azimuth = jnp.arange(phi_cells, dtype=jnp.float32) * (2.0 * math.pi / phi_cells)
    column = jnp.arange(2 * LMAX + 1)
    order_m = ((column + 1) // 2).astype(jnp.float32)
    phase = azimuth[:, None] * order_m[None, :]
    root_two = math.sqrt(2.0)
    return jnp.where(column[None, :] == 0, jnp.ones_like(phase), jnp.where(column[None, :] % 2 == 1, root_two * jnp.cos(phase), root_two * jnp.sin(phase)))

def one_field(density):
    shells, theta_rows, phi_cells = density.shape
    polar_angle = (jnp.arange(theta_rows, dtype=jnp.float32) + 0.5) * (math.pi / theta_rows)
    legendre = legendre_table(polar_angle)
    weights = jnp.sin(polar_angle) * (math.pi / theta_rows) * (2.0 * math.pi / phi_cells)
    fourier = fourier_table(phi_cells)
    spacing = (1.0 - INNER) / shells
    radius = INNER + (jnp.arange(shells, dtype=jnp.float32) + 0.5) * spacing
    azimuthal = jnp.dot(density.reshape(shells * theta_rows, phi_cells), fourier, precision=lax.Precision.HIGHEST, preferred_element_type=jnp.float32)
    azimuthal = azimuthal.reshape(shells, theta_rows, 2 * LMAX + 1)
    moments = jnp.einsum('rtk,tlk->rlk', azimuthal, legendre * weights[:, None, None], precision=lax.Precision.HIGHEST)
    degree = jnp.arange(LMAX + 1, dtype=jnp.float32)
    inner_terms = moments * (radius[:, None] ** (degree + 2.0) * spacing)[:, :, None]
    outer_terms = moments * (radius[:, None] ** (1.0 - degree) * spacing)[:, :, None]
    inner_sum = jnp.cumsum(inner_terms, 0) - 0.5 * inner_terms
    outer_sum = jnp.flip(jnp.cumsum(jnp.flip(outer_terms, 0), 0), 0) - 0.5 * outer_terms
    factor = (-COUPLING * 4.0 * math.pi / (2.0 * degree + 1.0))[None, :, None]
    coefficient = factor * (radius[:, None, None] ** (-(degree[None, :, None] + 1.0)) * inner_sum + radius[:, None, None] ** degree[None, :, None] * outer_sum)
    spread = jnp.einsum('rlk,tlk->rtk', coefficient, legendre, precision=lax.Precision.HIGHEST)
    potential = jnp.dot(spread.reshape(shells * theta_rows, 2 * LMAX + 1), fourier.T, precision=lax.Precision.HIGHEST, preferred_element_type=jnp.float32)
    return potential.reshape(shells, theta_rows, phi_cells)

def reference(density):
    return lax.map(one_field, density)
```

```python
import functools
import math

import jax
import jax.numpy as jnp
import numpy as np
from jax import lax
from jax.experimental import pallas as pl
from jax.experimental.pallas import tpu as pltpu
from jax.sharding import PartitionSpec as P

LMAX = 12
NPHI = 512
NTH = 256
NR = 1024
FIELDS = 3
HALF = NPHI // 2
INNER = 0.5
COUPLING = 2000.0
MESH = pl.DeviceIdType.MESH
F32 = jnp.float32
BF16 = jnp.bfloat16
LANES = 128

SHELLS = 64
ROWS = 32
NRAD = 16
NANG = 8
GROUP = SHELLS // NANG
STEP = 16
OUT_STEP = 16


def slots(parity):
    return [
        (l, k)
        for l in range(LMAX + 1)
        for k in range(2 * LMAX + 1)
        if (k + 1) // 2 <= l and ((k + 1) // 2) % 2 == parity
    ]


def legendre():
    theta = (np.arange(NTH) + 0.5) * (math.pi / NTH)
    c, s = np.cos(theta), np.sin(theta)
    v = {(0, 0): np.full_like(theta, 1.0 / math.sqrt(4.0 * math.pi))}
    for m in range(1, LMAX + 1):
        v[m, m] = math.sqrt((2.0 * m + 1.0) / (2.0 * m)) * s * v[m - 1, m - 1]
    for m in range(LMAX):
        v[m + 1, m] = math.sqrt(2.0 * m + 3.0) * c * v[m, m]
    for m in range(LMAX + 1):
        for l in range(m + 2, LMAX + 1):
            a = math.sqrt((4.0 * l * l - 1.0) / (l * l - m * m))
            b = math.sqrt(((l - 1.0) ** 2 - m * m) / (4.0 * (l - 1.0) ** 2 - 1.0))
            v[l, m] = a * (c * v[l - 1, m] - b * v[l - 2, m])
    weight = s * (math.pi / NTH) * (2.0 * math.pi / NPHI)
    return v, weight


def fourier():
    phi = np.arange(NPHI) * (2.0 * math.pi / NPHI)
    columns = [np.ones_like(phi)]
    for m in range(1, LMAX + 1):
        columns.append(math.sqrt(2.0) * np.cos(m * phi))
        columns.append(math.sqrt(2.0) * np.sin(m * phi))
    return columns


def hi_lo(table):
    hi = table.astype(np.float32).astype(BF16)
    lo = (table - hi.astype(np.float64)).astype(np.float32).astype(BF16)
    return hi, lo


def tables():
    v, weight = legendre()
    columns = fourier()
    forward = np.zeros((2, HALF, 2 * LANES), BF16)
    backward = np.zeros((2, 2 * LANES, HALF), BF16)
    moment = np.zeros((NTH, 2 * LANES), np.float32)
    spread = np.zeros((NTH, 4 * LANES), np.float32)
    misc = np.zeros((8, 2 * LANES), np.float32)
    misc[1] = 0.0
    for parity in range(2):
        used = slots(parity)
        n = len(used)
        f = np.stack([columns[k][:HALF] for _, k in used], -1)
        hi, lo = hi_lo(f)
        forward[parity, :, :n] = hi
        forward[parity, :, LANES : LANES + n] = lo
        backward[parity, :n] = hi.T
        backward[parity, 85 : 85 + n] = hi.T
        backward[parity, 170 : 170 + n] = lo.T
        table = np.stack([v[l, (k + 1) // 2] for l, k in used], -1)
        at = parity * LANES
        moment[:, at : at + n] = table * weight[:, None]
        for copy in range(3):
            start = 2 * at + 85 * copy
            spread[:, start : start + n] = table
        degree = np.array([l for l, _ in used], np.float64)
        misc[0, at : at + n] = degree
        misc[1, at : at + n] = -COUPLING * 4.0 * math.pi / (2.0 * degree + 1.0)
    return forward, backward, moment, spread, misc


def analyse(
    dens,
    forward,
    moment,
    misc,
    out,
    held,
    fwd,
    mom,
    mis,
    radial,
    part,
    got,
    mine,
    whole,
    tot_out,
    tot_in,
    car_out,
    car_in,
    dens_sem,
    tab_sem,
    rs_send,
    rs_recv,
    ag_send,
    ag_recv,
    tot_send,
    tot_recv,
    car_send,
    car_recv,
):
    me_r = lax.axis_index("rad")
    me_a = lax.axis_index("ang")
    steps = SHELLS // STEP

    def density_copy(f, c):
        at = pl.ds(c * STEP, STEP)
        return pltpu.make_async_copy(
            dens.at[f, at], held.at[f, at], dens_sem.at[f * steps + c]
        )

    first = pltpu.make_async_copy(forward, fwd, tab_sem.at[0])
    second = pltpu.make_async_copy(
        moment.at[pl.ds(pl.multiple_of(me_a * ROWS, ROWS), ROWS)], mom, tab_sem.at[1]
    )
    third = pltpu.make_async_copy(misc, mis, tab_sem.at[2])
    first.start()
    second.start()
    third.start()
    for f in range(FIELDS):
        for c in range(steps):
            density_copy(f, c).start()

    barrier = pltpu.get_barrier_semaphore()
    for d in range(1, NANG):
        pl.semaphore_signal(
            barrier,
            inc=1,
            device_id=(me_r, lax.rem(me_a + d, NANG)),
            device_id_type=MESH,
        )
    for d in range(1, NRAD):
        pl.semaphore_signal(
            barrier,
            inc=1,
            device_id=(lax.rem(me_r + d, NRAD), me_a),
            device_id_type=MESH,
        )

    third.wait()
    shell = lax.broadcasted_iota(jnp.int32, (SHELLS, 2 * LANES), 0) + me_r * SHELLS
    spacing = (1.0 - INNER) / NR
    radius = INNER + (shell.astype(F32) + 0.5) * spacing
    degree = mis[0:1, :]
    factor = mis[1:2, :]
    power = jnp.exp(degree * jnp.log(radius))
    inverse = 1.0 / power
    radial[0] = power * radius * radius * spacing
    radial[1] = inverse * radius * spacing
    radial[2] = factor * inverse / radius
    radial[3] = factor * power
    tot_in[me_r] = jnp.zeros((4, 2 * LANES), F32)
    tot_out[...] = jnp.zeros((2, 4, 2 * LANES), F32)
    first.wait()
    second.wait()
    pl.semaphore_wait(barrier, NANG + NRAD - 2)

    def rs_copy(f, d):
        peer = lax.rem(me_a + d, NANG)
        return pltpu.make_async_remote_copy(
            src_ref=part.at[f, peer],
            dst_ref=got.at[f, me_a],
            send_sem=rs_send.at[f, d],
            recv_sem=rs_recv.at[f, me_a],
            device_id=(me_r, peer),
            device_id_type=MESH,
        )

    def rs_arrival(f, d):
        source = lax.rem(me_a + d, NANG)
        return pltpu.make_async_remote_copy(
            src_ref=part.at[f, source],
            dst_ref=got.at[f, source],
            send_sem=rs_send.at[f, d],
            recv_sem=rs_recv.at[f, source],
            device_id=(me_r, source),
            device_id_type=MESH,
        )

    def ag_copy(f, d):
        peer = lax.rem(me_a + d, NANG)
        return pltpu.make_async_remote_copy(
            src_ref=mine.at[f],
            dst_ref=whole.at[f, me_a],
            send_sem=ag_send.at[f, d],
            recv_sem=ag_recv.at[f, me_a],
            device_id=(me_r, peer),
            device_id_type=MESH,
        )

    def ag_arrival(f, d):
        source = lax.rem(me_a + d, NANG)
        return pltpu.make_async_remote_copy(
            src_ref=mine.at[f],
            dst_ref=whole.at[f, source],
            send_sem=ag_send.at[f, d],
            recv_sem=ag_recv.at[f, source],
            device_id=(me_r, source),
            device_id_type=MESH,
        )

    def tot_copy(d):
        peer = lax.rem(me_r + d, NRAD)
        return pltpu.make_async_remote_copy(
            src_ref=tot_out.at[lax.div(me_r + d, NRAD)],
            dst_ref=tot_in.at[me_r],
            send_sem=tot_send.at[d],
            recv_sem=tot_recv.at[me_r],
            device_id=(peer, me_a),
            device_id_type=MESH,
        )

    def tot_arrival(d):
        source = lax.rem(me_r + d, NRAD)
        return pltpu.make_async_remote_copy(
            src_ref=tot_out.at[0],
            dst_ref=tot_in.at[source],
            send_sem=tot_send.at[d],
            recv_sem=tot_recv.at[source],
            device_id=(source, me_a),
            device_id_type=MESH,
        )

    def car_copy(d):
        peer = lax.rem(me_a + d, NANG)
        return pltpu.make_async_remote_copy(
            src_ref=car_out,
            dst_ref=car_in.at[me_a],
            send_sem=car_send.at[d],
            recv_sem=car_recv.at[me_a],
            device_id=(me_r, peer),
            device_id_type=MESH,
        )

    def car_arrival(d):
        source = lax.rem(me_a + d, NANG)
        return pltpu.make_async_remote_copy(
            src_ref=car_out,
            dst_ref=car_in.at[source],
            send_sem=car_send.at[d],
            recv_sem=car_recv.at[source],
            device_id=(me_r, source),
            device_id_type=MESH,
        )

    def snapshot(f, _):
        def chunk(c, _):
            density_copy(f, c).wait()
            x = held[f, pl.ds(c * STEP, STEP)].reshape(STEP * ROWS, NPHI)
            left, right = x[:, :HALF], x[:, HALF:]
            sums = []
            for parity in range(2):
                y = left + right if parity == 0 else left - right
                hi = y.astype(BF16)
                lo = (y - hi.astype(F32)).astype(BF16)
                weights = fwd[parity]
                p = jnp.dot(hi, weights, preferred_element_type=F32) + jnp.dot(
                    lo, weights, preferred_element_type=F32
                )
                a = (p[:, :LANES] + p[:, LANES:]).reshape(STEP, ROWS, LANES)
                w = mom[:, parity * LANES : (parity + 1) * LANES]
                sums.append(jnp.sum(a * w[None], 1))
            both = jnp.concatenate(sums, -1)
            part[f, pl.ds(c * (STEP // GROUP), STEP // GROUP)] = both.reshape(
                STEP // GROUP, GROUP, 2 * LANES
            )
            return 0

        lax.fori_loop(0, steps, chunk, 0)
        for d in range(1, NANG):
            rs_copy(f, d).start()
        moments = part[f].reshape(SHELLS, 2 * LANES)
        for side in range(2):
            tot_out[side, pl.ds(f, 1)] = jnp.sum(moments * radial[side], 0, keepdims=True)
        return 0

    lax.fori_loop(0, FIELDS, snapshot, 0)
    for d in range(1, NRAD):
        tot_copy(d).start()

    def reduce(f, _):
        total = part[f, me_a]
        for d in range(1, NANG):
            rs_arrival(f, d).wait_recv()
            total += got[f, lax.rem(me_a + d, NANG)]
        mine[f] = total
        whole[f, me_a] = total
        for d in range(1, NANG):
            ag_copy(f, d).start()
        return 0

    lax.fori_loop(0, FIELDS, reduce, 0)

    for d in range(1, NRAD):
        tot_arrival(d).wait_recv()
    below = jnp.zeros((4, 2 * LANES), F32)
    above = jnp.zeros((4, 2 * LANES), F32)
    for r in range(NRAD):
        term = tot_in[r]
        below += jnp.where(r < me_r, term, 0.0)
        above += jnp.where(r > me_r, term, 0.0)
    car_out[0] = below
    car_out[1] = above
    car_in[me_a, 0] = below
    car_in[me_a, 1] = above
    for d in range(1, NANG):
        car_copy(d).start()

    row = lax.broadcasted_iota(jnp.int32, (SHELLS, SHELLS), 0)
    col = lax.broadcasted_iota(jnp.int32, (SHELLS, SHELLS), 1)
    same = jnp.where(row == col, 0.5, 0.0)
    lower = (jnp.where(col < row, 1.0, 0.0) + same).astype(BF16)
    upper = (jnp.where(col > row, 1.0, 0.0) + same).astype(BF16)

    def running(triangle, terms):
        hi = terms.astype(BF16)
        rest = terms - hi.astype(F32)
        mid = rest.astype(BF16)
        lo = (rest - mid.astype(F32)).astype(BF16)
        total = jnp.dot(triangle, hi, preferred_element_type=F32)
        total += jnp.dot(triangle, mid, preferred_element_type=F32)
        return total + jnp.dot(triangle, lo, preferred_element_type=F32)

    def tripled(half):
        zeros = jnp.zeros((SHELLS, LANES), F32)
        wide = jnp.concatenate([half, zeros], -1)
        return wide + pltpu.roll(wide, 85, 1) + pltpu.roll(wide, 170, 1)

    def put(f, value):
        for parity in range(2):
            out[pl.ds(pl.multiple_of(f * SHELLS, SHELLS), SHELLS), pl.ds(parity * 2 * LANES, 2 * LANES)] = (
                tripled(value[:, parity * LANES : (parity + 1) * LANES])
            )

    for f in range(FIELDS):
        for d in range(1, NANG):
            ag_arrival(f, d).wait_recv()
        moments = whole[f].reshape(SHELLS, 2 * LANES)
        inner = running(lower, moments * radial[0])
        outer = running(upper, moments * radial[1])
        if f == 0:
            for d in range(1, NANG):
                car_arrival(d).wait_recv()
            carry = car_in[0]
            for a in range(1, NANG):
                carry += car_in[a]
        inner += carry[0, f : f + 1]
        outer += carry[1, f : f + 1]
        put(f, radial[2] * inner + radial[3] * outer)

    for f in range(FIELDS):
        for d in range(1, NANG):
            rs_copy(f, d).wait_send()
            ag_copy(f, d).wait_send()
    for d in range(1, NANG):
        car_copy(d).wait_send()
    for d in range(1, NRAD):
        tot_copy(d).wait_send()


def synthesise(coef, bwd, spread, out, held, out_sem):
    own = pl.ds(pl.multiple_of(lax.axis_index("ang") * ROWS, ROWS), ROWS)
    steps = FIELDS * SHELLS // OUT_STEP

    def out_copy(c):
        at = pl.ds(c * OUT_STEP, OUT_STEP)
        return pltpu.make_async_copy(held.at[at], out.at[at], out_sem.at[c])

    lane = lax.broadcasted_iota(jnp.int32, (OUT_STEP * ROWS, 2 * LANES), 1)
    keep = jnp.logical_and(lane >= 85, lane < 170)

    def chunk(c, _):
        z = []
        for parity in range(2):
            at = pl.ds(parity * 2 * LANES, 2 * LANES)
            row = coef[pl.ds(pl.multiple_of(c * OUT_STEP, OUT_STEP), OUT_STEP), at]
            x = (row[:, None, :] * spread[own, at][None]).reshape(OUT_STEP * ROWS, 2 * LANES)
            hi = x.astype(BF16).astype(F32)
            z.append(
                jnp.dot(
                    jnp.where(keep, x - hi, hi).astype(BF16),
                    bwd[parity],
                    preferred_element_type=F32,
                )
            )
        both = jnp.concatenate([z[0] + z[1], z[0] - z[1]], -1)
        held[pl.ds(c * OUT_STEP, OUT_STEP)] = both.reshape(OUT_STEP, ROWS, NPHI)
        out_copy(c).start()
        return 0

    lax.fori_loop(0, steps, chunk, 0)
    for c in range(steps):
        out_copy(c).wait()


def body(density):
    forward, backward, moment, spread, misc = tables()
    hbm = pl.BlockSpec(memory_space=pltpu.HBM)
    vmem = pl.BlockSpec(memory_space=pltpu.VMEM)
    dma = pltpu.SemaphoreType.DMA
    wide = 2 * LANES
    coef = pl.pallas_call(
        analyse,
        out_shape=jax.ShapeDtypeStruct((FIELDS * SHELLS, 4 * LANES), F32),
        in_specs=[hbm] * 4,
        out_specs=vmem,
        scratch_shapes=[
            pltpu.VMEM((FIELDS, SHELLS, ROWS, NPHI), F32),
            pltpu.VMEM((2, HALF, wide), BF16),
            pltpu.VMEM((ROWS, wide), F32),
            pltpu.VMEM((8, wide), F32),
            pltpu.VMEM((4, SHELLS, wide), F32),
            pltpu.VMEM((FIELDS, NANG, GROUP, wide), F32),
            pltpu.VMEM((FIELDS, NANG, GROUP, wide), F32),
            pltpu.VMEM((FIELDS, GROUP, wide), F32),
            pltpu.VMEM((FIELDS, NANG, GROUP, wide), F32),
            pltpu.VMEM((2, 4, wide), F32),
            pltpu.VMEM((NRAD, 4, wide), F32),
            pltpu.VMEM((2, 4, wide), F32),
            pltpu.VMEM((NANG, 2, 4, wide), F32),
            dma((FIELDS * SHELLS // STEP,)),
            dma((3,)),
            dma((FIELDS, NANG)),
            dma((FIELDS, NANG)),
            dma((FIELDS, NANG)),
            dma((FIELDS, NANG)),
            dma((NRAD,)),
            dma((NRAD,)),
            dma((NANG,)),
            dma((NANG,)),
        ],
        compiler_params=pltpu.CompilerParams(
            collective_id=0, has_side_effects=True, vmem_limit_bytes=40 << 20
        ),
        name="analyse",
    )(*[pltpu.with_memory_space_constraint(x, pltpu.HBM) for x in (density, jnp.asarray(forward), jnp.asarray(moment), jnp.asarray(misc))])
    potential = pl.pallas_call(
        synthesise,
        out_shape=jax.ShapeDtypeStruct((FIELDS * SHELLS, ROWS, NPHI), F32),
        in_specs=[vmem, vmem, vmem],
        out_specs=hbm,
        scratch_shapes=[
            pltpu.VMEM((FIELDS * SHELLS, ROWS, NPHI), F32),
            dma((FIELDS * SHELLS // OUT_STEP,)),
        ],
        compiler_params=pltpu.CompilerParams(vmem_limit_bytes=40 << 20),
        name="synthesise",
    )(coef, jnp.asarray(backward), jnp.asarray(spread))
    return potential.reshape(FIELDS, SHELLS, ROWS, NPHI)


def solution(mesh):
    return jax.shard_map(
        body,
        mesh=mesh,
        in_specs=(P(None, "rad", "ang", None),),
        out_specs=P(None, "rad", "ang", None),
        check_vma=False,
    )
```

```python
import functools
import math

import jax
import jax.numpy as jnp
import numpy as np
from jax import lax
from jax.experimental import pallas as pl
from jax.experimental.pallas import tpu as pltpu
from jax.sharding import PartitionSpec as P

LMAX = 12
NPHI = 512
NTH = 256
NR = 1024
FIELDS = 3
HALF = NPHI // 2
INNER = 0.5
COUPLING = 2000.0
MESH = pl.DeviceIdType.MESH
F32 = jnp.float32
BF16 = jnp.bfloat16
LANES = 128

SHELLS = 64
ROWS = 32
NRAD = 16
NANG = 8
GROUP = SHELLS // NANG
STEP = 32
AHEAD = 2
OUT_STEP = 16
SPLIT = 85


def slots(parity):
    return [
        (l, k)
        for l in range(LMAX + 1)
        for k in range(2 * LMAX + 1)
        if (k + 1) // 2 <= l and ((k + 1) // 2) % 2 == parity
    ]


def legendre():
    theta = (np.arange(NTH) + 0.5) * (math.pi / NTH)
    c, s = np.cos(theta), np.sin(theta)
    v = {(0, 0): np.full_like(theta, 1.0 / math.sqrt(4.0 * math.pi))}
    for m in range(1, LMAX + 1):
        v[m, m] = math.sqrt((2.0 * m + 1.0) / (2.0 * m)) * s * v[m - 1, m - 1]
    for m in range(LMAX):
        v[m + 1, m] = math.sqrt(2.0 * m + 3.0) * c * v[m, m]
    for m in range(LMAX + 1):
        for l in range(m + 2, LMAX + 1):
            a = math.sqrt((4.0 * l * l - 1.0) / (l * l - m * m))
            b = math.sqrt(((l - 1.0) ** 2 - m * m) / (4.0 * (l - 1.0) ** 2 - 1.0))
            v[l, m] = a * (c * v[l - 1, m] - b * v[l - 2, m])
    weight = s * (math.pi / NTH) * (2.0 * math.pi / NPHI)
    return v, weight


def fourier():
    phi = np.arange(NPHI) * (2.0 * math.pi / NPHI)
    columns = [np.ones_like(phi)]
    for m in range(1, LMAX + 1):
        columns.append(math.sqrt(2.0) * np.cos(m * phi))
        columns.append(math.sqrt(2.0) * np.sin(m * phi))
    return columns


def hi_lo(table):
    hi = table.astype(np.float32).astype(BF16)
    lo = (table - hi.astype(np.float64)).astype(np.float32).astype(BF16)
    return hi, lo


def tables():
    v, weight = legendre()
    columns = fourier()
    forward = np.zeros((2, HALF, 2 * LANES), BF16)
    backward = np.zeros((2, 2 * LANES, HALF), BF16)
    moment = np.zeros((NTH, 2 * LANES), np.float32)
    spread = np.zeros((NTH, 4 * LANES), np.float32)
    misc = np.zeros((8, 2 * LANES), np.float32)
    rest = LANES - SPLIT
    for parity in range(2):
        used = slots(parity)
        n = len(used)
        f = np.stack([columns[k][:HALF] for _, k in used], -1)
        hi, lo = hi_lo(f)
        forward[parity, :, :n] = hi
        forward[parity, :, LANES : LANES + n] = lo
        table = np.stack([v[l, (k + 1) // 2] for l, k in used], -1)
        at = parity * LANES
        moment[:, at : at + n] = table * weight[:, None]
        for half in range(2):
            row = half * LANES
            backward[parity, row : row + n] = hi.T
            part = slice(0, rest) if half == 0 else slice(rest, n)
            size = part.stop - part.start
            backward[parity, row + SPLIT : row + SPLIT + size] = lo.T[part]
            lane = 2 * at + row
            spread[:, lane : lane + n] = table
            spread[:, lane + SPLIT : lane + SPLIT + size] = table[:, part]
        degree = np.array([l for l, _ in used], np.float64)
        misc[0, at : at + n] = degree
        misc[1, at : at + n] = -COUPLING * 4.0 * math.pi / (2.0 * degree + 1.0)
    local = np.concatenate(
        [
            moment.reshape(NANG, ROWS, 2 * LANES),
            np.broadcast_to(misc, (NANG, 8, 2 * LANES)),
        ],
        1,
    )
    return forward, backward, local, spread


def widened(value):
    lane = lax.broadcasted_iota(jnp.int32, (value.shape[0], LANES), 1)
    pieces = []
    for parity in range(2):
        half = value[:, parity * LANES : (parity + 1) * LANES]
        pieces.append(jnp.where(lane < SPLIT, half, pltpu.roll(half, SPLIT, 1)))
        pieces.append(jnp.where(lane < SPLIT, half, pltpu.roll(half, 2 * SPLIT - LANES, 1)))
    return jnp.concatenate(pieces, -1)


def analyse(
    dens,
    forward,
    local,
    out,
    held,
    fwd,
    loc,
    radial,
    radial_wide,
    part,
    got,
    mine,
    whole,
    base,
    tot_out,
    tot_in,
    car_out,
    car_in,
    dens_sem,
    tab_sem,
    rs_recv,
    ag_recv,
    tot_recv,
    car_recv,
    send_sem,
):
    me_r = lax.axis_index("rad")
    me_a = lax.axis_index("ang")
    steps = SHELLS // STEP
    total_steps = FIELDS * steps
    others = pl.ds(0, NANG - 1)

    def density_copy(g):
        f, c = lax.div(g, steps), lax.rem(g, steps)
        at = pl.ds(c * STEP, STEP)
        return pltpu.make_async_copy(
            dens.at[f, at], held.at[f, at], dens_sem.at[lax.rem(g, AHEAD + 1)]
        )

    second = pltpu.make_async_copy(local.at[me_a], loc, tab_sem.at[0])
    first = pltpu.make_async_copy(forward, fwd, tab_sem.at[1])
    second.start()
    first.start()
    for g in range(AHEAD):
        density_copy(jnp.int32(g)).start()

    barrier = pltpu.get_barrier_semaphore()
    for d in range(1, NANG):
        pl.semaphore_signal(
            barrier,
            inc=1,
            device_id=(me_r, lax.rem(me_a + d, NANG)),
            device_id_type=MESH,
        )
    for d in range(1, NRAD):
        pl.semaphore_signal(
            barrier,
            inc=1,
            device_id=(lax.rem(me_r + d, NRAD), me_a),
            device_id_type=MESH,
        )

    def send(src, dst, k, recv, rad, ang):
        return pltpu.make_async_remote_copy(
            src_ref=src,
            dst_ref=dst,
            send_sem=send_sem.at[k],
            recv_sem=recv,
            device_id=(rad, ang),
            device_id_type=MESH,
        )

    def ang_peer(d):
        return lax.rem(me_a + d, NANG)

    def rad_peer(d):
        return lax.rem(me_r + d, NRAD)

    shell = lax.broadcasted_iota(jnp.int32, (SHELLS, 2 * LANES), 0) + me_r * SHELLS
    spacing = (1.0 - INNER) / NR
    radius = INNER + (shell.astype(F32) + 0.5) * spacing
    log_radius = jnp.log(radius)
    tot_in[me_r] = jnp.zeros((4, 2 * LANES), F32)
    tot_out[...] = jnp.zeros((2, 4, 2 * LANES), F32)
    second.wait()
    degree = loc[ROWS : ROWS + 1, :]
    factor = loc[ROWS + 1 : ROWS + 2, :]
    power = jnp.exp(degree * log_radius)
    inverse = 1.0 / power
    radial[0] = power * radius * radius * spacing
    radial[1] = inverse * radius * spacing
    below_weight = factor * inverse / radius
    above_weight = factor * power
    radial[2] = below_weight
    radial[3] = above_weight
    radial_wide[0] = widened(below_weight)
    radial_wide[1] = widened(above_weight)
    first.wait()

    def snapshot(f, _):
        def chunk(c, _):
            g = f * steps + c
            density_copy(g).wait()

            @pl.when(g + AHEAD < total_steps)
            def _():
                density_copy(g + AHEAD).start()

            x = held[f, pl.ds(c * STEP, STEP)].reshape(STEP * ROWS, NPHI)
            left, right = x[:, :HALF], x[:, HALF:]
            sums = []
            for parity in range(2):
                y = left + right if parity == 0 else left - right
                hi = y.astype(BF16)
                lo = (y - hi.astype(F32)).astype(BF16)
                weights = fwd[parity]
                p = jnp.dot(hi, weights, preferred_element_type=F32) + jnp.dot(
                    lo, weights, preferred_element_type=F32
                )
                a = (p[:, :LANES] + p[:, LANES:]).reshape(STEP, ROWS, LANES)
                w = loc[:ROWS, parity * LANES : (parity + 1) * LANES]
                sums.append(jnp.sum(a * w[None], 1))
            both = jnp.concatenate(sums, -1)
            part[f, pl.ds(c * (STEP // GROUP), STEP // GROUP)] = both.reshape(
                STEP // GROUP, GROUP, 2 * LANES
            )
            return 0

        lax.fori_loop(0, steps, chunk, 0)
        moments = part[f].reshape(SHELLS, 2 * LANES)
        for side in range(2):
            tot_out[side, pl.ds(f, 1)] = jnp.sum(moments * radial[side], 0, keepdims=True)

        @pl.when(f == 0)
        def _():
            pl.semaphore_wait(barrier, NANG + NRAD - 2)

        @pl.when(f == FIELDS - 1)
        def _():
            for d in range(1, NRAD):
                send(
                    tot_out.at[lax.div(me_r + d, NRAD)],
                    tot_in.at[me_r],
                    2,
                    tot_recv.at[0],
                    rad_peer(d),
                    me_a,
                ).start()

        for d in range(1, NANG):
            send(
                part.at[f, ang_peer(d)], got.at[f, me_a], 0, rs_recv.at[f], me_r, ang_peer(d)
            ).start()
        got[f, me_a] = part[f, me_a]
        return 0

    lax.fori_loop(0, FIELDS, snapshot, 0)

    def reduce(f, _):
        send(
            part.at[f, others], got.at[f, others], 0, rs_recv.at[f], me_r, ang_peer(1)
        ).wait_recv()
        total = jnp.sum(got[f], 0)
        mine[f] = total
        whole[f, me_a] = total
        for d in range(1, NANG):
            send(
                mine.at[f], whole.at[f, me_a], 1, ag_recv.at[f], me_r, ang_peer(d)
            ).start()
        return 0

    lax.fori_loop(0, FIELDS, reduce, 0)

    arrived = pl.ds(0, NRAD - 1)
    send(
        tot_in.at[arrived], tot_in.at[arrived], 2, tot_recv.at[0], rad_peer(1), me_a
    ).wait_recv()
    below = jnp.zeros((4, 2 * LANES), F32)
    above = jnp.zeros((4, 2 * LANES), F32)
    for r in range(NRAD):
        term = tot_in[r]
        below += jnp.where(r < me_r, term, 0.0)
        above += jnp.where(r > me_r, term, 0.0)
    car_out[0] = below
    car_out[1] = above
    for d in range(1, NANG):
        send(car_out, car_in.at[me_a], 3, car_recv.at[0], me_r, ang_peer(d)).start()
    car_in[me_a, 0] = below
    car_in[me_a, 1] = above

    row = lax.broadcasted_iota(jnp.int32, (SHELLS, SHELLS), 0)
    col = lax.broadcasted_iota(jnp.int32, (SHELLS, SHELLS), 1)
    same = jnp.where(row == col, 0.5, 0.0)
    lower = (jnp.where(col < row, 1.0, 0.0) + same).astype(BF16)
    upper = (jnp.where(col > row, 1.0, 0.0) + same).astype(BF16)

    def running(triangle, terms):
        hi = terms.astype(BF16)
        rest = terms - hi.astype(F32)
        mid = rest.astype(BF16)
        lo = (rest - mid.astype(F32)).astype(BF16)
        total = jnp.dot(triangle, hi, preferred_element_type=F32)
        total += jnp.dot(triangle, mid, preferred_element_type=F32)
        return total + jnp.dot(triangle, lo, preferred_element_type=F32)

    def local_sums(f, _):
        send(
            whole.at[f, others], whole.at[f, others], 1, ag_recv.at[f], me_r, ang_peer(1)
        ).wait_recv()
        moments = whole[f].reshape(SHELLS, 2 * LANES)
        inner = running(lower, moments * radial[0])
        outer = running(upper, moments * radial[1])
        base[f] = widened(radial[2] * inner + radial[3] * outer)
        return 0

    lax.fori_loop(0, FIELDS, local_sums, 0)
    send(car_in.at[others], car_in.at[others], 3, car_recv.at[0], me_r, ang_peer(1)).wait_recv()
    carry = car_in[0]
    for a in range(1, NANG):
        carry += car_in[a]
    below = widened(carry[0])
    above = widened(carry[1])
    for f in range(FIELDS):
        out[f * SHELLS : (f + 1) * SHELLS] = (
            base[f] + radial_wide[0] * below[f : f + 1] + radial_wide[1] * above[f : f + 1]
        )

    send(
        part.at[:, others], got.at[:, others], 0, rs_recv.at[0], me_r, ang_peer(1)
    ).wait_send()
    send(
        whole.at[:, others], whole.at[:, others], 1, rs_recv.at[0], me_r, ang_peer(1)
    ).wait_send()
    send(
        tot_in.at[arrived], tot_in.at[arrived], 2, tot_recv.at[0], rad_peer(1), me_a
    ).wait_send()
    send(car_in.at[others], car_in.at[others], 3, car_recv.at[0], me_r, ang_peer(1)).wait_send()


def synthesise(coef, bwd, spread, out, held, out_sem):
    own = pl.ds(pl.multiple_of(lax.axis_index("ang") * ROWS, ROWS), ROWS)
    steps = FIELDS * SHELLS // OUT_STEP
    lane = lax.broadcasted_iota(jnp.int32, (OUT_STEP * ROWS, LANES), 1)

    def chunk(c, _):
        rows = pl.ds(pl.multiple_of(c * OUT_STEP, OUT_STEP), OUT_STEP)
        z = []
        for parity in range(2):
            pieces = []
            for half in range(2):
                at = pl.ds((2 * parity + half) * LANES, LANES)
                x = coef[rows, at][:, None, :] * spread[own, at][None]
                x = x.reshape(OUT_STEP * ROWS, LANES)
                hi = x.astype(BF16)
                if half == 1:
                    hi = hi.astype(F32)
                    hi = jnp.where(lane < SPLIT, x - hi, hi).astype(BF16)
                pieces.append(hi)
            z.append(
                jnp.dot(
                    jnp.concatenate(pieces, -1), bwd[parity], preferred_element_type=F32
                )
            )
        both = jnp.concatenate([z[0] + z[1], z[0] - z[1]], -1)
        held[rows] = both.reshape(OUT_STEP, ROWS, NPHI)
        pltpu.make_async_copy(held.at[rows], out.at[rows], out_sem.at[0]).start()
        return 0

    lax.fori_loop(0, steps, chunk, 0)
    pltpu.make_async_copy(held, out, out_sem.at[0]).wait()


def body(density):
    forward, backward, local, spread = (jnp.asarray(t) for t in tables())
    hbm = pl.BlockSpec(memory_space=pltpu.HBM)
    vmem = pl.BlockSpec(memory_space=pltpu.VMEM)
    dma = pltpu.SemaphoreType.DMA
    wide = 2 * LANES
    coef = pl.pallas_call(
        analyse,
        out_shape=jax.ShapeDtypeStruct((FIELDS * SHELLS, 2 * wide), F32),
        in_specs=[hbm] * 3,
        out_specs=vmem,
        scratch_shapes=[
            pltpu.VMEM((FIELDS, SHELLS, ROWS, NPHI), F32),
            pltpu.VMEM((2, HALF, wide), BF16),
            pltpu.VMEM((ROWS + 8, wide), F32),
            pltpu.VMEM((4, SHELLS, wide), F32),
            pltpu.VMEM((2, SHELLS, 2 * wide), F32),
            pltpu.VMEM((FIELDS, NANG, GROUP, wide), F32),
            pltpu.VMEM((FIELDS, NANG, GROUP, wide), F32),
            pltpu.VMEM((FIELDS, GROUP, wide), F32),
            pltpu.VMEM((FIELDS, NANG, GROUP, wide), F32),
            pltpu.VMEM((FIELDS, SHELLS, 2 * wide), F32),
            pltpu.VMEM((2, 4, wide), F32),
            pltpu.VMEM((NRAD, 4, wide), F32),
            pltpu.VMEM((2, 4, wide), F32),
            pltpu.VMEM((NANG, 2, 4, wide), F32),
            dma((AHEAD + 1,)),
            dma((2,)),
            dma((FIELDS,)),
            dma((FIELDS,)),
            dma((1,)),
            dma((1,)),
            dma((4,)),
        ],
        compiler_params=pltpu.CompilerParams(
            collective_id=0, has_side_effects=True, vmem_limit_bytes=40 << 20
        ),
        name="analyse",
    )(*[pltpu.with_memory_space_constraint(x, pltpu.HBM) for x in (density, forward, local)])
    potential = pl.pallas_call(
        synthesise,
        out_shape=jax.ShapeDtypeStruct((FIELDS * SHELLS, ROWS, NPHI), F32),
        in_specs=[vmem, vmem, vmem],
        out_specs=hbm,
        scratch_shapes=[
            pltpu.VMEM((FIELDS * SHELLS, ROWS, NPHI), F32),
            dma((1,)),
        ],
        compiler_params=pltpu.CompilerParams(vmem_limit_bytes=40 << 20),
        name="synthesise",
    )(coef, backward, spread)
    return potential.reshape(FIELDS, SHELLS, ROWS, NPHI)


def solution(mesh):
    return jax.shard_map(
        body,
        mesh=mesh,
        in_specs=(P(None, "rad", "ang", None),),
        out_specs=P(None, "rad", "ang", None),
        check_vma=False,
    )
```
